512 devices in a mesh: samp: 64 (over x, z, y_lo), tgt: 8 (over y_hi, core).
Axes of the slice: x: 4, y: 8 (y_hi: 4, y_lo: 2; y = y_hi * 2 + y_lo), z: 8, core: 2. Of those that a mesh axis runs over, the one named last changes fastest.
Arguments:
- samples: bfloat16 [12288, 128], P('samp'), may hold values from -6 to 6
- omega: bfloat16 [128, 4096], replicated, may hold values from -0.5 to 0.5
- phase: float32 [4096], replicated, may hold values from -3.140625 to 3.140625
- right_side: float32 [4096, 512], P('samp', 'tgt'), may hold values from -6 to 6
Outputs:
- weights: float32 [4096, 512], P('samp', 'tgt')
The draws below stay inside these ranges and needn't reach their ends.
All inputs are finite; a program needn't handle non-finite values.
Results may differ from the reference program's by a relative error of at most 0.011.
The reference program's roundings to bfloat16 on the way count: a program that leaves them out, or rounds other values in their place, can miss the bound.
Values may be sent and summed in bfloat16 or wider, within the bound.
A program may use at most 128 MiB of HBM per device.

```python
import jax
import jax.numpy as jnp
from jax import lax

F = 4096
K = 512
DX = 128
ITERS = 2
N = 12288


def steps_of(rng, shape, shards, least, top_value):
    factor_of = 1.0
    for dim, blocks in shards:
        heights = jax.random.uniform(jax.random.fold_in(jax.random.fold_in(rng, 6), dim), (blocks,), jnp.float32, least / len(shards), top_value / len(shards))
        factor_of = factor_of * jnp.repeat(jnp.exp(heights), shape[dim] // blocks).reshape((-1,) + (1,) * (len(shape) - 1 - dim))
    return factor_of


def gaussian(rng, shape, deviation, bound, shards=(), held_as=jnp.bfloat16):
    values = jax.random.normal(rng, shape, jnp.float32) * deviation
    if len(shards) > 0:
        values = steps_of(rng, shape, shards, -0.22, 0.18) * values
    return jnp.clip(values, min=-bound, max=bound).astype(held_as)


def setup_inputs(seed: int = 0) -> dict:
    streams_of = jax.random.split(jax.random.key(seed), 5)
    return {
        "samples": gaussian(streams_of[0], (N, DX), 1.0, 6.0, ((0, 64),)),
        "omega": gaussian(streams_of[1], (DX, F), DX ** -0.5, 0.5),
        "phase": jnp.clip(jax.random.uniform(streams_of[2], (F,), jnp.float32, -3.140625, 3.140625), -3.140625, 3.140625),
        "right_side": gaussian(streams_of[3], (F, K), 1.0, 6.0, ((0, 64), (1, 8)), jnp.float32),
    }


ridge = 1.0

def precise_dot(left_matrix, right_matrix):
    return jnp.dot(left_matrix, right_matrix, precision=lax.Precision.HIGHEST)

def spd_solve(gram_matrix, rhs_matrix):
    factor = jnp.linalg.cholesky(gram_matrix)
    return jax.scipy.linalg.cho_solve((factor, True), rhs_matrix)

def reference(samples, omega, phase, right_side):
    preact = jnp.dot(samples.astype(jnp.float32), omega.astype(jnp.float32), preferred_element_type=jnp.float32) + phase
    features = jnp.cos(preact).astype(jnp.bfloat16)
    sample_total = features.shape[0]
    weights = jnp.zeros_like(right_side)
    residual = right_side
    direction = right_side
    gram_rr = precise_dot(residual.T, residual)
    for iteration in range(ITERS):
        projected = jnp.dot(features.astype(jnp.float32), direction.astype(jnp.bfloat16).astype(jnp.float32), preferred_element_type=jnp.float32).astype(jnp.bfloat16)
        image = jnp.dot(features.T.astype(jnp.float32), projected.astype(jnp.float32), preferred_element_type=jnp.float32) / sample_total + ridge * direction
        alpha_coef = spd_solve(precise_dot(direction.T, image), gram_rr)
        weights = weights + precise_dot(direction, alpha_coef)
        residual = residual - precise_dot(image, alpha_coef)
        gram_new = precise_dot(residual.T, residual)
        beta_coef = spd_solve(gram_rr, gram_new)
        direction = residual + precise_dot(direction, beta_coef)
        gram_rr = gram_new
    return weights
```

```python
import jax
import jax.numpy as jnp
from jax import lax
from jax.experimental import pallas as pl
from jax.experimental.pallas import tpu as pltpu
from jax.sharding import PartitionSpec as P

f32 = jnp.float32
bf16 = jnp.bfloat16
MESH = pl.DeviceIdType.MESH
VMEM = pl.BlockSpec(memory_space=pltpu.VMEM)
RIDGE = 1.0

NX, NZ, NY, NU, NC = 4, 8, 2, 4, 2
COLS = 64
PAIR = 128
SLOTS = NX * NZ
CHUNK = 24
GRAM = CHUNK * NZ
TOTAL = NU * NC * COLS
BK = 128
PN = 8
NT = (((1,), (1,)), ((), ()))
NN = (((1,), (0,)), ((), ()))


def fine(a, b, dims=NN):
    return lax.dot_general(a, b, dims, precision=lax.Precision.HIGHEST, preferred_element_type=f32)


def quick(a, b, dims=NN):
    return lax.dot_general(a, b, dims, preferred_element_type=f32)


class Place:
    def __init__(self, send_sem, recv_sem):
        samp, tgt = lax.axis_index("samp"), lax.axis_index("tgt")
        self.x, self.z, self.y = samp // 16, (samp % 16) // 2, samp % 2
        self.u, self.c = tgt // 2, tgt % 2
        self.slot = self.x * NZ + self.z
        self.send_sem, self.recv_sem, self.used = send_sem, recv_sem, 0

    def at(self, x=None, z=None, y=None, u=None, c=None):
        x, z, y = (own if new is None else new for own, new in ((self.x, x), (self.z, z), (self.y, y)))
        u, c = (own if new is None else new for own, new in ((self.u, u), (self.c, c)))
        return (x * 16 + z * 2 + y, u * 2 + c)

    def z_peers(self):
        return [lax.rem(self.z + d, NZ) for d in range(1, NZ)]

    def x_peers(self):
        return [lax.rem(self.x + d, NX) for d in range(1, NX)]

    def u_peers(self):
        return [lax.rem(self.u + d, NU) for d in range(1, NU)]

    def xy_peers(self):
        return [(lax.rem(self.x + d, NX), y) for d in range(NX) for y in (self.y, 1 - self.y)][1:]

    def greet(self):
        devices = [self.at(z=z) for z in self.z_peers()]
        devices += [self.at(x=x, y=y) for x, y in self.xy_peers()]
        devices += [self.at(u=u) for u in self.u_peers()] + [self.at(c=1 - self.c)]
        barrier = pltpu.get_barrier_semaphore()
        for device in devices:
            pl.semaphore_signal(barrier, inc=1, device_id=device, device_id_type=MESH)
        pl.semaphore_wait(barrier, len(devices))

    def send(self, src, dst, device):
        index = self.used
        self.used += 1
        copy = pltpu.make_async_remote_copy(
            src_ref=src,
            dst_ref=dst,
            send_sem=self.send_sem.at[index],
            recv_sem=self.recv_sem.at[index],
            device_id=device,
            device_id_type=MESH,
        )
        copy.start()
        return copy


def finish(copies):
    for copy in copies:
        copy.wait()


def run(*works):
    works = list(works)
    while works:
        works = [work for work in works if next(work, "end") != "end"]


def gather_slots(here, block, parts):
    rest = block
    for part in parts:
        part[here.slot] = rest.astype(bf16)
        rest = rest - rest.astype(bf16).astype(f32)
    along_z = [[here.send(p.at[here.slot], p.at[here.slot], here.at(z=z)) for z in here.z_peers()] for p in parts]
    yield
    along_x = []
    for p, copies in zip(parts, along_z):
        finish(copies)
        own = p.at[pl.ds(here.x * NZ, NZ)]
        along_x.append([here.send(own, own, here.at(x=x)) for x in here.x_peers()])
    for copies in along_x:
        yield
        finish(copies)


def gather_targets(here, ref):
    own = ref.at[here.u, here.c]
    copies = [here.send(own, own, here.at(u=u)) for u in here.u_peers()]
    yield
    finish(copies)
    own = ref.at[:, here.c]
    copies = [here.send(own, own, here.at(c=1 - here.c))]
    yield
    finish(copies)


def gram_sum(here, part, out, from_z, from_xy):
    copies = [
        here.send(part.at[pl.ds(z * CHUNK, CHUNK)], from_z.at[i], here.at(z=z)) for i, z in enumerate(here.z_peers())
    ]
    yield
    finish(copies)
    rows = pl.ds(pl.multiple_of(here.z * CHUNK, CHUNK), CHUNK)
    total = part[rows]
    for i in range(NZ - 1):
        total = total + from_z[i]
    index = here.x * NY + here.y
    from_xy[index] = total
    copies = [here.send(from_xy.at[index], from_xy.at[index], here.at(x=x, y=y)) for x, y in here.xy_peers()]
    yield
    finish(copies)
    total = from_xy[0]
    for i in range(1, NX * NY):
        total = total + from_xy[i]
    out[here.u, here.c, rows] = total
    own = out.at[here.u, here.c, rows]
    copies = [here.send(own, own, here.at(u=u)) for u in here.u_peers()]
    yield
    finish(copies)
    own = out.at[:, here.c, rows]
    copies = [here.send(own, own, here.at(z=z)) for z in here.z_peers()]
    yield
    finish(copies)
    own = out.at[:, here.c]
    copies = [here.send(own, own, here.at(c=1 - here.c))]
    yield
    finish(copies)


def gram_share(here, left, right):
    mask = lax.broadcasted_iota(jnp.int32, (COLS, PAIR), 1) // COLS == here.y
    whole = right[here.u].reshape(NC * COLS, PAIR)
    shares = []
    for d in range(3):
        rows = left[lax.rem(here.u + d, NU), here.c]
        shares.append(fine(jnp.where(mask, rows, 0.0), whole, NT))
    return jnp.concatenate(shares, axis=0)


def project(slots, feats, ref):
    samples = feats.shape[0]
    ref[...] = jnp.zeros_like(ref)

    def one(i, carry):
        at = pl.ds(pl.multiple_of(i * PAIR, PAIR), PAIR)
        return carry + quick(slots[i], feats[:, at], NT)

    total = lax.fori_loop(0, SLOTS, one, jnp.zeros((COLS, samples), f32))
    ref[:, :samples] = total


def first_kernel(
    total_samples, feats, block, b_all, q_all, t_all, gram_s, gram_m,
    from_y, high, low, proj, proj_low, t_err, share_s, share_m, sz, sxy, mz, mxy, image, image_x, image_z, sum_x, sum_z, image_y,
    send_sem, recv_sem,
):
    here = Place(send_sem, recv_sem)
    samples = feats.shape[0]
    here.greet()
    copy = here.send(block, from_y, here.at(y=1 - here.y))
    copy.wait()
    b_all[here.u, here.c] = block[...] + from_y[...]

    def gram_of_start():
        yield from gather_targets(here, b_all)
        share_m[...] = gram_share(here, b_all, b_all)
        yield from gram_sum(here, share_m, gram_m, mz, mxy)

    sum_of_start = gram_of_start()
    gathering = gather_slots(here, b_all[here.u, here.c], (high, low))
    next(sum_of_start)
    next(gathering)
    next(gathering)
    next(sum_of_start)
    next(gathering)
    project(high, feats, proj)
    t_all[here.u, here.c] = proj[...].astype(bf16)
    targets_t = gather_targets(here, t_all)
    next(targets_t)
    next(sum_of_start)

    rounded = proj[:, :samples].astype(bf16)

    def one(i, carry):
        at = pl.ds(pl.multiple_of(i * PAIR, PAIR), PAIR)
        image[i] = quick(rounded, feats[:, at]).astype(bf16)
        return carry

    lax.fori_loop(0, SLOTS, one, 0)

    def sum_of_image():
        copies = [
            here.send(image.at[pl.ds(x * NZ, NZ)], image_x.at[i], here.at(x=x)) for i, x in enumerate(here.x_peers())
        ]
        yield
        finish(copies)
        total = image[pl.ds(here.x * NZ, NZ)].astype(f32)
        for i in range(NX - 1):
            total = total + image_x[i].astype(f32)
        sum_x[...] = total
        copies = [here.send(sum_x.at[z], image_z.at[i], here.at(z=z)) for i, z in enumerate(here.z_peers())]
        yield
        finish(copies)
        total = sum_x[here.z]
        for i in range(NZ - 1):
            total = total + image_z[i]
        sum_z[...] = total
        copies = [here.send(sum_z, image_y, here.at(y=1 - here.y))]
        yield
        finish(copies)
        total = sum_z[...] + image_y[...]
        q_all[here.u, here.c] = total * (1.0 / total_samples) + RIDGE * b_all[here.u, here.c]
        yield from gather_targets(here, q_all)

    def gram_of_image():
        yield from gathering
        project(low, feats, proj_low)
        t_err[here.u, here.c] = (proj[...] - proj[...].astype(bf16).astype(f32) + proj_low[...]).astype(bf16)
        targets_e = gather_targets(here, t_err)
        next(targets_e)
        next(targets_t)
        yield
        yield from targets_e
        next(targets_t, None)
        right = t_all[here.u].reshape(NC * COLS, -1)
        right_err = t_err[here.u].reshape(NC * COLS, -1)
        shares = []
        for d in range(3):
            at = lax.rem(here.u + d, NU)
            value, err = t_all[at, here.c], t_err[at, here.c]
            cross = quick(err, right, NT) + quick(value, right_err, NT)
            shares.append(quick(value, right, NT) + 0.5 * cross)
        gram = jnp.concatenate(shares, axis=0) * (1.0 / total_samples)
        share_s[...] = gram + RIDGE * share_m[...]
        yield from gram_sum(here, share_s, gram_s, sz, sxy)

    run(gram_of_image(), sum_of_image(), sum_of_start)


def second_kernel(feats, r_all, v_all, gram_r, high, proj, share, rz, rxy, send_sem, recv_sem):
    here = Place(send_sem, recv_sem)
    here.greet()
    share[...] = gram_share(here, r_all, r_all)

    def targets():
        yield from gather_slots(here, r_all[here.u, here.c], (high,))
        project(high, feats, proj)
        v_all[here.u, here.c] = proj[...].astype(bf16)
        yield from gather_targets(here, v_all)

    run(gram_sum(here, share, gram_r, rz, rxy), targets())


def third_kernel(share, gram_p, pz, pxy, send_sem, recv_sem):
    here = Place(send_sem, recv_sem)
    here.greet()
    run(gram_sum(here, share, gram_p, pz, pxy))


def invert_blocks(blocks):
    count = BK // PN
    row = lax.broadcasted_iota(jnp.int32, (PN, BK), 0)
    lane = lax.broadcasted_iota(jnp.int32, (PN, BK), 1)
    mats = [[b[g * PN : (g + 1) * PN, :] for g in range(count)] for b in blocks]

    def wide(v, j):
        return jnp.broadcast_to(v[:, j : j + 1], (PN, BK))

    def tall(v, i):
        return jnp.broadcast_to(v[i : i + 1, :], (PN, BK))

    for p in range(count):
        base = p * PN
        inside = (lane >= base) & (lane < base + PN)
        reduced = []
        for m in mats:
            panel = m[p]
            cols = [wide(panel, base + k) for k in range(PN)]
            for i in range(PN):
                inv = 1.0 / tall(cols[i], i)
                here = row == i
                factor = jnp.where(here, 0.0, cols[i])
                src = jnp.where(lane == base + i, jnp.where(here, 1.0, 0.0), panel)
                pivot = tall(src, i) * inv
                panel = jnp.where(here, pivot, src - factor * pivot)
                for k in range(i + 1, PN):
                    top = tall(cols[k], i) * inv
                    cols[k] = jnp.where(here, top, cols[k] - factor * top)
            reduced.append(panel)
        for m, panel in zip(mats, reduced):
            rows = [tall(panel, k) for k in range(PN)]
            for g in [(p + 1 + g) % count for g in range(count - 1)]:
                acc = jnp.where(inside, 0.0, m[g])
                for k in range(PN):
                    acc = acc - wide(m[g], base + k) * rows[k]
                m[g] = acc
            m[p] = panel
    return [jnp.concatenate(m, axis=0) for m in mats]


def invert(refs):
    steps = TOTAL // BK
    eye = jnp.where(
        lax.broadcasted_iota(jnp.int32, (BK, BK), 0) == lax.broadcasted_iota(jnp.int32, (BK, BK), 1), 1.0, 0.0
    )

    def one(k, carry):
        at = pl.ds(pl.multiple_of(k * BK, BK), BK)
        inverses = invert_blocks([ref[at, at] for ref in refs])
        for ref, inverse in zip(refs, inverses):
            ref[at, at] = eye
            head = fine(inverse, ref[at, :])
            for d in range(1, steps):
                i = lax.rem(k + d, steps)
                ai = pl.ds(pl.multiple_of(i * BK, BK), BK)
                left = ref[ai, at]
                ref[ai, at] = jnp.zeros((BK, BK), f32)
                ref[ai, :] = ref[ai, :] - fine(left, head)
            ref[at, :] = head
        return carry

    lax.fori_loop(0, steps, one, 0)


def assemble(gram, ref):
    for u in range(NU):
        for d in range(3):
            r = (u + d) % NU
            block = gram[u, :, d * COLS : (d + 1) * COLS, :].reshape(BK, BK)
            ref[r * BK : (r + 1) * BK, u * BK : (u + 1) * BK] = block
            if d == 1:
                ref[u * BK : (u + 1) * BK, r * BK : (r + 1) * BK] = block.T


def alpha_kernel(gram_s, gram_m, b_all, q_all, m_inv, alpha_t, r_all, s_inv, m_full):
    assemble(gram_s, s_inv)
    assemble(gram_m, m_full)
    m_inv[...] = m_full[...]
    invert([s_inv, m_inv])
    alpha_t[...] = fine(m_full[...], s_inv[...])
    r_all[...] = b_all[...] - fine(alpha_t[...], q_all[...])


def beta_kernel(total_samples, gram_r, m_inv, r_all, b_all, v_all, t_all, p_all, r_full, share, t1, beta_t):
    tgt = lax.axis_index("tgt")
    y = lax.axis_index("samp") % 2
    u, c = tgt // 2, tgt % 2
    assemble(gram_r, r_full)
    beta_t[...] = fine(r_full[...], m_inv[...])
    p_all[...] = r_all[...] + fine(beta_t[...], b_all[...])
    t1[...] = (v_all[...].astype(f32) + fine(beta_t[...], t_all[...].astype(f32))).astype(bf16)
    mask = lax.broadcasted_iota(jnp.int32, (COLS, PAIR), 1) // COLS == y
    own = pl.ds(pl.multiple_of(u * 2 * COLS, 2 * COLS), 2 * COLS)
    right_p, right_t = p_all[own, :], t1[own, :]
    for d in range(3):
        at = pl.ds(pl.multiple_of((lax.rem(u + d, NU) * 2 + c) * COLS, COLS), COLS)
        gram = quick(t1[at, :], right_t, NT) * (1.0 / total_samples)
        share[d * COLS : (d + 1) * COLS, :] = gram + RIDGE * fine(jnp.where(mask, p_all[at, :], 0.0), right_p, NT)


def weight_kernel(gram_p, r_full, alpha_t, b_all, p_all, out, p_inv):
    tgt = lax.axis_index("tgt")
    y = lax.axis_index("samp") % 2
    own = pl.ds(pl.multiple_of(tgt * COLS, COLS), COLS)
    assemble(gram_p, p_inv)
    invert([p_inv])
    last_t = fine(r_full[own, :], p_inv[...])
    weights = fine(alpha_t[own, :], b_all[...]) + fine(last_t, p_all[...])
    mine = jnp.where(y == 0, weights[:, :COLS], weights[:, COLS:])
    out[...] = mine.T


def shape(dims, dtype=f32):
    return jax.ShapeDtypeStruct(dims, dtype)


def call(kernel, name, args, outs, scratch, collective_id=None):
    params = dict(vmem_limit_bytes=60 * 2**20)
    if collective_id is not None:
        params.update(collective_id=collective_id, has_side_effects=True)
    return pl.pallas_call(
        kernel,
        out_shape=outs,
        in_specs=[VMEM] * len(args),
        out_specs=[VMEM] * len(outs),
        scratch_shapes=scratch,
        name=name,
        compiler_params=pltpu.CompilerParams(**params),
    )(*args)


def copies(count):
    return [pltpu.SemaphoreType.DMA((count,))] * 2


def body(samples, omega, phase, right_side):
    count = samples.shape[0]
    lanes = 2 * PAIR
    total_samples = count * lax.axis_size("samp")
    y = lax.axis_index("samp") % 2
    preact = jnp.dot(samples, omega, preferred_element_type=f32) + phase
    feats = jnp.cos(preact).astype(bf16)
    turned = right_side.T
    zero = jnp.zeros_like(turned)
    block = jnp.concatenate([jnp.where(y == 0, turned, zero), jnp.where(y == 1, turned, zero)], axis=1)

    vm = pltpu.VMEM
    all_feats = (NU, NC, COLS, PAIR)
    all_samples = (NU, NC, COLS, lanes)
    gram = (NU, NC, GRAM, BK)
    sums = [vm((NZ - 1, CHUNK, BK), f32), vm((NX * NY, CHUNK, BK), f32)]
    slots = vm((SLOTS, COLS, PAIR), bf16)
    b_all, q_all, t_all, gram_s, gram_m = call(
        lambda *refs: first_kernel(total_samples, *refs),
        "first",
        (feats, block),
        [shape(all_feats), shape(all_feats), shape(all_samples, bf16), shape(gram), shape(gram)],
        [
            vm((COLS, PAIR), f32), slots, slots, vm((COLS, lanes), f32), vm((COLS, lanes), f32), vm(all_samples, bf16),
            vm((GRAM, BK), f32), vm((GRAM, BK), f32), *sums, *sums,
            slots, vm((NX - 1, NZ, COLS, PAIR), bf16), vm((NZ - 1, COLS, PAIR), f32),
            vm((NZ, COLS, PAIR), f32), vm((COLS, PAIR), f32), vm((COLS, PAIR), f32),
        ]
        + copies(104),
        1,
    )
    flat = (TOTAL, PAIR)
    full = (TOTAL, TOTAL)
    b_flat = b_all.reshape(flat)
    m_inv, alpha_t, r_all = call(
        alpha_kernel,
        "alpha",
        (gram_s, gram_m, b_flat, q_all.reshape(flat)),
        [shape(full), shape(full), shape(flat)],
        [vm(full, f32), vm(full, f32)],
    )
    v_all, gram_r = call(
        second_kernel,
        "second",
        (feats, r_all.reshape(all_feats)),
        [shape(all_samples, bf16), shape(gram)],
        [slots, vm((COLS, lanes), f32), vm((GRAM, BK), f32), *sums] + copies(48),
        2,
    )
    p_all, r_full, share = call(
        lambda *refs: beta_kernel(total_samples, *refs),
        "beta",
        (gram_r, m_inv, r_all, b_flat, v_all.reshape(TOTAL, lanes), t_all.reshape(TOTAL, lanes)),
        [shape(flat), shape(full), shape((GRAM, BK))],
        [vm((TOTAL, lanes), bf16), vm(full, f32)],
    )
    (gram_p,) = call(third_kernel, "third", (share,), [shape(gram)], sums + copies(32), 3)
    (out,) = call(
        weight_kernel, "weight", (gram_p, r_full, alpha_t, b_flat, p_all), [shape((COLS, COLS))], [vm(full, f32)]
    )
    return out


def solution(mesh):
    placed = (P("samp", None), P(), P(), P("samp", "tgt"))
    return jax.shard_map(body, mesh=mesh, in_specs=placed, out_specs=P("samp", "tgt"), check_vma=False)
```

```python
import jax
import jax.numpy as jnp
from jax import lax
from jax.experimental import pallas as pl
from jax.experimental.pallas import tpu as pltpu
from jax.sharding import PartitionSpec as P

f32 = jnp.float32
bf16 = jnp.bfloat16
MESH = pl.DeviceIdType.MESH
VMEM = pl.BlockSpec(memory_space=pltpu.VMEM)
RIDGE = 1.0

NX, NZ, NY, NU, NC = 4, 8, 2, 4, 2
COLS = 64
PAIR = 128
SLOTS = NX * NZ
CHUNK = 24
GRAM = CHUNK * NZ
TOTAL = NU * NC * COLS
BK = 128
PN = 8
COPIES = 200
NT = (((1,), (1,)), ((), ()))
NN = (((1,), (0,)), ((), ()))


def fine(a, b, dims=NN):
    return lax.dot_general(a, b, dims, precision=lax.Precision.HIGHEST, preferred_element_type=f32)


def quick(a, b, dims=NN):
    return lax.dot_general(a, b, dims, preferred_element_type=f32)


class Place:
    def __init__(self, send_sem, recv_sem):
        samp, tgt = lax.axis_index("samp"), lax.axis_index("tgt")
        self.x, self.z, self.y = samp // 16, (samp % 16) // 2, samp % 2
        self.u, self.c = tgt // 2, tgt % 2
        self.slot = self.x * NZ + self.z
        self.send_sem, self.recv_sem, self.used = send_sem, recv_sem, 0

    def at(self, x=None, z=None, y=None, u=None, c=None):
        x, z, y = (own if new is None else new for own, new in ((self.x, x), (self.z, z), (self.y, y)))
        u, c = (own if new is None else new for own, new in ((self.u, u), (self.c, c)))
        return (x * 16 + z * 2 + y, u * 2 + c)

    def z_peers(self):
        return [lax.rem(self.z + d, NZ) for d in range(1, NZ)]

    def x_peers(self):
        return [lax.rem(self.x + d, NX) for d in range(1, NX)]

    def u_peers(self):
        return [lax.rem(self.u + d, NU) for d in range(1, NU)]

    def xy_peers(self):
        return [(lax.rem(self.x + d, NX), y) for d in range(NX) for y in (self.y, 1 - self.y)][1:]

    def greet(self):
        devices = [self.at(z=z) for z in self.z_peers()]
        devices += [self.at(x=x, y=y) for x, y in self.xy_peers()]
        devices += [self.at(u=u) for u in self.u_peers()] + [self.at(c=1 - self.c)]
        barrier = pltpu.get_barrier_semaphore()
        for device in devices:
            pl.semaphore_signal(barrier, inc=1, device_id=device, device_id_type=MESH)
        self.greeted = len(devices)

    def meet(self):
        pl.semaphore_wait(pltpu.get_barrier_semaphore(), self.greeted)

    def step(self, make):
        return Step(self, make)


class Step:
    def __init__(self, here, make):
        self.here, self.make = here, make
        self.first = here.used
        here.used += len(make())

    def copies(self):
        return [
            pltpu.make_async_remote_copy(
                src_ref=src,
                dst_ref=dst,
                send_sem=self.here.send_sem.at[self.first + i],
                recv_sem=self.here.recv_sem.at[self.first + i],
                device_id=device,
                device_id_type=MESH,
            )
            for i, (src, dst, device) in enumerate(self.make())
        ]

    def start(self):
        for copy in self.copies():
            copy.start()

    def wait(self):
        for copy in self.copies():
            copy.wait()


def run(*works):
    works = list(works)
    while works:
        works = [work for work in works if next(work, "end") != "end"]


def gather_slots(here, part):
    along_z = here.step(
        lambda: [(part.at[here.slot], part.at[here.slot], here.at(z=z)) for z in here.z_peers()]
    )
    along_z.start()
    yield
    along_z.wait()

    def to_x():
        own = part.at[pl.ds(here.x * NZ, NZ)]
        return [(own, own, here.at(x=x)) for x in here.x_peers()]

    along_x = here.step(to_x)
    along_x.start()
    yield
    along_x.wait()


def gather_near(here, ref):
    def near():
        own = ref.at[here.u, here.c]
        return [(own, own, here.at(u=u)) for u in here.u_peers()] + [(own, own, here.at(c=1 - here.c))]

    step = here.step(near)
    step.start()
    yield
    step.wait()


def swap_rest(here, ref):
    def rest():
        copies = []
        for u in here.u_peers():
            block = ref.at[u, here.c]
            copies.append((block, block, here.at(c=1 - here.c)))
        return copies

    step = here.step(rest)
    step.start()
    yield
    step.wait()


def gather_targets(here, ref):
    yield from gather_near(here, ref)
    yield from swap_rest(here, ref)


def gram_sum(here, part, out, from_z, from_xy):
    spread = here.step(
        lambda: [
            (part.at[pl.ds(z * CHUNK, CHUNK)], from_z.at[i], here.at(z=z)) for i, z in enumerate(here.z_peers())
        ]
    )
    spread.start()
    yield
    spread.wait()
    total = part[pl.ds(pl.multiple_of(here.z * CHUNK, 8), CHUNK)]
    for i in range(NZ - 1):
        total = total + from_z[i]
    from_xy[here.x * NY + here.y] = total

    def to_xy():
        own = from_xy.at[here.x * NY + here.y]
        return [(own, own, here.at(x=x, y=y)) for x, y in here.xy_peers()]

    across = here.step(to_xy)
    across.start()
    yield
    across.wait()
    total = from_xy[0]
    for i in range(1, NX * NY):
        total = total + from_xy[i]
    out[here.u, here.c, pl.ds(pl.multiple_of(here.z * CHUNK, 8), CHUNK)] = total

    def to_u():
        own = out.at[here.u, here.c, pl.ds(here.z * CHUNK, CHUNK)]
        return [(own, own, here.at(u=u)) for u in here.u_peers()]

    along_u = here.step(to_u)
    along_u.start()
    yield
    along_u.wait()

    def to_z():
        own = out.at[:, here.c, pl.ds(here.z * CHUNK, CHUNK)]
        return [(own, own, here.at(z=z)) for z in here.z_peers()]

    along_z = here.step(to_z)
    along_z.start()
    yield
    along_z.wait()
    swap = here.step(lambda: [(out.at[:, here.c], out.at[:, here.c], here.at(c=1 - here.c))])
    swap.start()
    yield
    swap.wait()


def gram_share(here, left, right):
    mask = lax.broadcasted_iota(jnp.int32, (COLS, PAIR), 1) // COLS == here.y
    whole = right[here.u].reshape(NC * COLS, PAIR)
    shares = []
    for d in range(3):
        rows = left[lax.rem(here.u + d, NU), here.c]
        shares.append(fine(jnp.where(mask, rows, 0.0), whole, NT))
    return jnp.concatenate(shares, axis=0)


def project(slots, feats, first, count):
    def group(i, total):
        index = lax.rem(first + i, NX)
        for z in range(NZ):
            at = pl.ds(pl.multiple_of((index * NZ + z) * PAIR, PAIR), PAIR)
            total = total + quick(slots[index * NZ + z], feats[:, at], NT)
        return total

    return lax.fori_loop(0, count, group, jnp.zeros((COLS, feats.shape[0]), f32))


def cosine(x):
    n = jnp.floor(x * 0.3183098861837907 + 0.5)
    r = ((x - n * 3.140625) - n * 0.0009670257568359375) - n * 6.2771141529083251953e-07
    half = n * 0.5
    sign = 1.0 - 4.0 * (half - jnp.floor(half))
    q = r * r
    poly = 1.0 / 479001600.0
    for term in (-1.0 / 3628800.0, 1.0 / 40320.0, -1.0 / 720.0, 1.0 / 24.0, -0.5, 1.0):
        poly = poly * q + term
    return sign * poly


def invert_blocks(blocks):
    count = BK // PN
    row = lax.broadcasted_iota(jnp.int32, (PN, BK), 0)
    lane = lax.broadcasted_iota(jnp.int32, (PN, BK), 1)
    mats = [[b[g * PN : (g + 1) * PN, :] for g in range(count)] for b in blocks]

    def wide(v, j):
        return jnp.broadcast_to(v[:, j : j + 1], (PN, BK))

    def tall(v, i):
        return jnp.broadcast_to(v[i : i + 1, :], (PN, BK))

    for p in range(count):
        base = p * PN
        inside = (lane >= base) & (lane < base + PN)
        reduced = []
        for m in mats:
            panel = m[p]
            cols = [wide(panel, base + k) for k in range(PN)]
            for i in range(PN):
                inv = 1.0 / tall(cols[i], i)
                here = row == i
                factor = jnp.where(here, 0.0, cols[i])
                src = jnp.where(lane == base + i, jnp.where(here, 1.0, 0.0), panel)
                pivot = tall(src, i) * inv
                panel = jnp.where(here, pivot, src - factor * pivot)
                for k in range(i + 1, PN):
                    top = tall(cols[k], i) * inv
                    cols[k] = jnp.where(here, top, cols[k] - factor * top)
            reduced.append(panel)
        for m, panel in zip(mats, reduced):
            rows = [tall(panel, k) for k in range(PN)]
            for g in [(p + 1 + g) % count for g in range(count - 1)]:
                acc = jnp.where(inside, 0.0, m[g])
                for k in range(PN):
                    acc = acc - wide(m[g], base + k) * rows[k]
                m[g] = acc
            m[p] = panel
    return [jnp.concatenate(m, axis=0) for m in mats]


def reduce_block(ref, k, at, hook):
    (inverse,) = invert_blocks([ref[at, at]])
    ref[at, at] = inverse
    hook()
    inverse = ref[at, at]
    rows = lax.broadcasted_iota(jnp.int32, (TOTAL, BK), 0)
    cols = lax.broadcasted_iota(jnp.int32, (BK, BK), 1)
    ref[at, at] = jnp.where(lax.broadcasted_iota(jnp.int32, (BK, BK), 0) == cols, 1.0, 0.0)
    head = fine(inverse, ref[at, :])
    left = jnp.where(rows // BK == k, 0.0, ref[:, at])
    ref[:, at] = jnp.zeros((TOTAL, BK), f32)
    ref[...] = ref[...] - fine(left, head)
    ref[at, :] = head


def invert(ref, hooks=None):
    steps = TOTAL // BK
    if hooks is None:

        def one(k, carry):
            reduce_block(ref, k, pl.ds(pl.multiple_of(k * BK, BK), BK), lambda: None)
            return carry

        lax.fori_loop(0, steps, one, 0)
    else:
        for k in range(steps):
            reduce_block(ref, k, pl.ds(k * BK, BK), hooks[2 * k])
            hooks[2 * k + 1]()


def assemble(gram, ref):
    for u in range(NU):
        for d in range(3):
            r = (u + d) % NU
            block = gram[u, :, d * COLS : (d + 1) * COLS, :].reshape(BK, BK)
            ref[r * BK : (r + 1) * BK, u * BK : (u + 1) * BK] = block
            if d == 1:
                ref[u * BK : (u + 1) * BK, r * BK : (r + 1) * BK] = block.T


def later(*works):
    def hook():
        for work in works:
            next(work, None)

    return hook


def kernel(
    total_samples, samples, omega, phase, right_side, out,
    feats, block, from_y, b_all, q_all, r_all, t_all, t_err, v_all, high, low, high_r, proj, image, image_x, image_z, sum_x,
    sum_z, image_y, share_m, share_s, share_r, share_p, gram_sm, gram_r, gram_p, mz, mxy, sz, sxy, rz, rxy,
    pz, pxy, inv_sm, p_inv, m_high, m_low, m_full, r_full, alpha_t, beta_t, p_all, t1, send_sem, recv_sem,
):
    here = Place(send_sem, recv_sem)
    count, lanes = samples.shape[0], t_all.shape[-1]
    flat = (TOTAL, PAIR)
    here.greet()
    mine = lax.broadcasted_iota(jnp.int32, (COLS, PAIR), 1) // COLS == here.y
    turned = right_side[...].T
    block[...] = jnp.where(mine, jnp.concatenate([turned, turned], axis=1), 0.0)

    def features(first, chunks):
        width = 2 * PAIR

        def one(i, carry):
            at = pl.ds(pl.multiple_of((first + i) * width, width), width)
            feats[:, at] = cosine(quick(samples[...], omega[:, at]) + phase[:, at]).astype(bf16)
            return carry

        lax.fori_loop(0, chunks, one, 0)

    scope = jax.named_scope
    gram_s, gram_m = gram_sm.at[0], gram_sm.at[1]
    s_inv, m_inv = inv_sm.at[0], inv_sm.at[1]
    with scope("feat1"):
        features(0, 8)
    with scope("meet"):
        here.meet()
    pair = here.step(lambda: [(block, from_y, here.at(y=1 - here.y))])
    pair.start()
    with scope("feat2"):
        features(8, 4)
        t_all[...] = jnp.zeros_like(t_all)
        t_err[...] = jnp.zeros_like(t_err)
        v_all[...] = jnp.zeros_like(v_all)
    with scope("pairwait"):
        pair.wait()
        both = block[...] + from_y[...]
        b_all[here.u, here.c] = both
        high[here.slot] = both.astype(bf16)
        low[here.slot] = (both - both.astype(bf16).astype(f32)).astype(bf16)
    gather_high, gather_low = gather_slots(here, high), gather_slots(here, low)
    targets_b = gather_near(here, b_all)
    next(gather_high)
    next(targets_b)
    next(gather_low)
    with scope("feat3"):
        features(12, 4)
    with scope("waithz"):
        next(gather_high)
    with scope("proj1"):
        proj[...] = project(high, feats, here.x, 1)
    with scope("waitlz"):
        next(gather_low)
    with scope("waitb"):
        next(targets_b, None)
    rest_b = swap_rest(here, b_all)
    with scope("sharem"):
        share_m[...] = gram_share(here, b_all, b_all)
    sum_m = gram_sum(here, share_m, gram_m, mz, mxy)
    next(sum_m)
    next(rest_b)
    with scope("waithx"):
        next(gather_high, None)
    with scope("proj2"):
        proj[...] = proj[...] + project(high, feats, here.x + 1, NX - 1)
        t_all[here.u, here.c, :, :count] = proj[...].astype(bf16)
    targets_t = gather_near(here, t_all)
    next(targets_t)
    with scope("m_z"):
        next(sum_m)

    with scope("image"):
        rounded = proj[...].astype(bf16)

        def image_group(i, carry):
            for z in range(NZ):
                at = pl.ds(pl.multiple_of((i * NZ + z) * PAIR, PAIR), PAIR)
                image[i * NZ + z] = quick(rounded, feats[:, at]).astype(bf16)
            return carry

        lax.fori_loop(0, NX, image_group, 0)

    def sum_of_image():
        def to_x():
            return [
                (image.at[pl.ds(x * NZ, NZ)], image_x.at[i], here.at(x=x)) for i, x in enumerate(here.x_peers())
            ]

        along_x = here.step(to_x)
        along_x.start()
        yield
        along_x.wait()
        total = image[pl.ds(here.x * NZ, NZ)].astype(f32)
        for i in range(NX - 1):
            total = total + image_x[i].astype(f32)
        sum_x[...] = total
        along_z = here.step(
            lambda: [(sum_x.at[z], image_z.at[i], here.at(z=z)) for i, z in enumerate(here.z_peers())]
        )
        along_z.start()
        yield
        along_z.wait()
        total = sum_x[here.z]
        for i in range(NZ - 1):
            total = total + image_z[i]
        sum_z[...] = total
        along_y = here.step(lambda: [(sum_z, image_y, here.at(y=1 - here.y))])
        along_y.start()
        yield
        along_y.wait()
        total = sum_z[...] + image_y[...]
        q_all[here.u, here.c] = total * (1.0 / total_samples) + RIDGE * b_all[here.u, here.c]
        yield from gather_targets(here, q_all)

    with scope("m_xy"):
        next(sum_m)
    with scope("waitlx"):
        next(gather_low, None)
    with scope("proj3"):
        exact = proj[...] + project(low, feats, 0, NX)
        t_err[here.u, here.c, :, :count] = (exact - proj[...].astype(bf16).astype(f32)).astype(bf16)
    targets_e = gather_near(here, t_err)
    next(targets_e)
    image_sum = sum_of_image()
    next(image_sum)
    with scope("m_u"):
        next(sum_m)
    with scope("waitt"):
        next(targets_t, None)
    with scope("waite"):
        next(targets_e, None)
    with scope("shares"):
        right = t_all[here.u].reshape(NC * COLS, lanes)
        right_err = t_err[here.u].reshape(NC * COLS, lanes)
        for d in range(3):
            at = lax.rem(here.u + d, NU)
            value, err = t_all[at, here.c], t_err[at, here.c]
            cross = quick(err, right, NT) + quick(value, right_err, NT)
            rows = pl.ds(d * COLS, COLS)
            share_s[rows] = (quick(value, right, NT) + 0.5 * cross) * (1.0 / total_samples) + RIDGE * share_m[rows]
    sum_s = gram_sum(here, share_s, gram_s, sz, sxy)
    next(sum_s)
    rest_t = swap_rest(here, t_all)
    next(rest_t)
    with scope("s_z"):
        next(sum_s)
    with scope("s_xy"):
        next(sum_s)
    with scope("m_z2"):
        next(sum_m)
    with scope("s_u"):
        next(sum_s)
    with scope("m_end"):
        next(sum_m, None)
    with scope("s_z2"):
        next(sum_s)
    with scope("s_end"):
        next(sum_s, None)

    mine_inv = inv_sm.at[here.c]
    with scope("assemble"):
        assemble(gram_sm.at[here.c], mine_inv)
    side, idle = later(image_sum), later()
    with scope("inverse1"):
        invert(mine_inv, [side, idle, side, side, idle, side, side, idle])
    swap = here.step(lambda: [(inv_sm.at[here.c], inv_sm.at[here.c], here.at(c=1 - here.c))])
    swap.start()
    with scope("drain"):
        run(rest_b, rest_t, image_sum)
        assemble(gram_m, m_full)
    with scope("swap"):
        swap.wait()
    with scope("alpha"):
        alpha_t[...] = fine(m_full[...], s_inv[...])
    with scope("resid"):
        residual = b_all[...].reshape(flat) - fine(alpha_t[...], q_all[...].reshape(flat))
        r_all[...] = residual.reshape(r_all.shape)
        high_r[here.slot] = r_all[here.u, here.c].astype(bf16)
    gather_r = gather_slots(here, high_r)
    next(gather_r)
    with scope("sharer"):
        share_r[...] = gram_share(here, r_all, r_all)
    sum_r = gram_sum(here, share_r, gram_r, rz, rxy)
    next(sum_r)
    with scope("m_split"):
        m_high[...] = m_inv[...].astype(bf16)
        m_low[...] = (m_inv[...] - m_high[...].astype(f32)).astype(bf16)
    with scope("r_gz"):
        next(gather_r)
    with scope("r_z"):
        next(sum_r)
    with scope("r_xy"):
        next(sum_r)
    with scope("r_gx"):
        next(gather_r, None)
    with scope("proj4"):
        v_all[here.u, here.c, :, :count] = project(high_r, feats, 0, NX).astype(bf16)
    gather_v = gather_targets(here, v_all)
    next(gather_v)
    with scope("r_u"):
        next(sum_r)
    with scope("v_u"):
        next(gather_v)
    with scope("r_z2"):
        next(sum_r)
    with scope("r_end"):
        run(sum_r, gather_v)

    with scope("beta"):
        assemble(gram_r, r_full)
        upper = r_full[...].astype(bf16)
        lower = (r_full[...] - upper.astype(f32)).astype(bf16)
        beta_t[...] = quick(upper, m_high[...]) + (quick(lower, m_high[...]) + quick(upper, m_low[...]))
    with scope("pdir"):
        p_all[...] = r_all[...].reshape(flat) + fine(beta_t[...], b_all[...].reshape(flat))
    with scope("tdir"):
        t_flat = t_all[...].reshape(TOTAL, lanes)
        upper = beta_t[...].astype(bf16)
        lower = (beta_t[...] - upper.astype(f32)).astype(bf16)
        moved = quick(upper, t_flat) + quick(lower, t_flat)
        t1[...] = (v_all[...].reshape(TOTAL, lanes).astype(f32) + moved).astype(bf16)
    with scope("sharep"):
        own = pl.ds(pl.multiple_of(here.u * 2 * COLS, 2 * COLS), 2 * COLS)
        right_p, right_t = p_all[own, :], t1[own, :]
        for d in range(3):
            at = pl.ds(pl.multiple_of((lax.rem(here.u + d, NU) * 2 + here.c) * COLS, COLS), COLS)
            gram = quick(t1[at, :], right_t, NT) * (1.0 / total_samples)
            share_p[pl.ds(d * COLS, COLS)] = gram + RIDGE * fine(jnp.where(mine, p_all[at, :], 0.0), right_p, NT)
    with scope("sump"):
        sum_p = gram_sum(here, share_p, gram_p, pz, pxy)
        next(sum_p)
        own = pl.ds(pl.multiple_of((here.u * 2 + here.c) * COLS, COLS), COLS)
        weights = fine(alpha_t[own, :], b_all[...].reshape(flat))
        run(sum_p)
    with scope("inverse2"):
        assemble(gram_p, p_inv)
        invert(p_inv)
    with scope("final"):
        last_t = fine(r_full[own, :], p_inv[...])
        weights = weights + fine(last_t, p_all[...])
        out[...] = jnp.where(here.y == 0, weights[:, :COLS], weights[:, COLS:]).T


def body(samples, omega, phase, right_side):
    count = samples.shape[0]
    total_samples = count * lax.axis_size("samp")
    vm = pltpu.VMEM
    all_feats = vm((NU, NC, COLS, PAIR), f32)
    all_samples = vm((NU, NC, COLS, 2 * PAIR), bf16)
    share = vm((GRAM, BK), f32)
    gram = vm((NU, NC, GRAM, BK), f32)
    sums = [vm((NZ - 1, CHUNK, BK), f32), vm((NX * NY, CHUNK, BK), f32)]
    slots = vm((SLOTS, COLS, PAIR), bf16)
    block = vm((COLS, PAIR), f32)
    full, half = vm((TOTAL, TOTAL), f32), vm((TOTAL, TOTAL), bf16)
    grams, fulls = vm((2, NU, NC, GRAM, BK), f32), vm((2, TOTAL, TOTAL), f32)
    scratch = [vm((count, omega.shape[1]), bf16), block, block, all_feats, all_feats, all_feats]
    scratch += [all_samples, all_samples, all_samples, slots, slots, slots, vm((COLS, count), f32)]
    scratch += [slots, vm((NX - 1, NZ, COLS, PAIR), bf16), vm((NZ - 1, COLS, PAIR), f32), vm((NZ, COLS, PAIR), f32)]
    scratch += [block, block, share, share, share, share, grams, gram, gram, *sums, *sums, *sums, *sums]
    scratch += [fulls, full, half, half, full, full, full, full, vm((TOTAL, PAIR), f32), vm((TOTAL, 2 * PAIR), bf16)]
    scratch += [pltpu.SemaphoreType.DMA((COPIES,))] * 2
    return pl.pallas_call(
        lambda *refs: kernel(total_samples, *refs),
        out_shape=jax.ShapeDtypeStruct(right_side.shape, f32),
        in_specs=[VMEM] * 4,
        out_specs=VMEM,
        scratch_shapes=scratch,
        name="cg",
        compiler_params=pltpu.CompilerParams(vmem_limit_bytes=60 * 2**20, collective_id=1, has_side_effects=True),
    )(samples, omega, phase.reshape(1, -1), right_side)


def solution(mesh):
    placed = (P("samp", None), P(), P(), P("samp", "tgt"))
    return jax.shard_map(body, mesh=mesh, in_specs=placed, out_specs=P("samp", "tgt"), check_vma=False)
```

```python
import jax
import jax.numpy as jnp
from jax import lax
from jax.experimental import pallas as pl
from jax.experimental.pallas import tpu as pltpu
from jax.sharding import PartitionSpec as P

f32 = jnp.float32
bf16 = jnp.bfloat16
MESH = pl.DeviceIdType.MESH
VMEM = pl.BlockSpec(memory_space=pltpu.VMEM)
RIDGE = 1.0

NX, NZ, NY, NU, NC = 4, 8, 2, 4, 2
COLS = 64
PAIR = 128
SLOTS = NX * NZ
CHUNK = 24
GRAM = CHUNK * NX * NY
TOTAL = NU * NC * COLS
BK = 128
PN = 8
COPIES = 200
NT = (((1,), (1,)), ((), ()))
NN = (((1,), (0,)), ((), ()))


def fine(a, b, dims=NN):
    return lax.dot_general(a, b, dims, precision=lax.Precision.HIGHEST, preferred_element_type=f32)


def quick(a, b, dims=NN):
    return lax.dot_general(a, b, dims, preferred_element_type=f32)


class Place:
    def __init__(self, send_sem, recv_sem):
        samp, tgt = lax.axis_index("samp"), lax.axis_index("tgt")
        self.x, self.z, self.y = samp // 16, (samp % 16) // 2, samp % 2
        self.u, self.c = tgt // 2, tgt % 2
        self.slot = self.x * NZ + self.z
        self.send_sem, self.recv_sem, self.used = send_sem, recv_sem, 0

    def at(self, x=None, z=None, y=None, u=None, c=None):
        x, z, y = (own if new is None else new for own, new in ((self.x, x), (self.z, z), (self.y, y)))
        u, c = (own if new is None else new for own, new in ((self.u, u), (self.c, c)))
        return (x * 16 + z * 2 + y, u * 2 + c)

    def z_peers(self):
        return [lax.rem(self.z + d, NZ) for d in range(1, NZ)]

    def x_peers(self):
        return [lax.rem(self.x + d, NX) for d in range(1, NX)]

    def u_peers(self):
        return [lax.rem(self.u + d, NU) for d in range(1, NU)]

    def xy_peers(self):
        return [(lax.rem(self.x + d, NX), y) for d in range(NX) for y in (self.y, 1 - self.y)][1:]

    def greet(self):
        devices = [self.at(z=z) for z in self.z_peers()]
        devices += [self.at(x=x, y=y) for x, y in self.xy_peers()]
        devices += [self.at(u=u) for u in self.u_peers()] + [self.at(c=1 - self.c)]
        barrier = pltpu.get_barrier_semaphore()
        for device in devices:
            pl.semaphore_signal(barrier, inc=1, device_id=device, device_id_type=MESH)
        self.greeted = len(devices)

    def meet(self):
        pl.semaphore_wait(pltpu.get_barrier_semaphore(), self.greeted)

    def step(self, make):
        return Step(self, make)


class Step:
    def __init__(self, here, make):
        self.here, self.make = here, make
        self.first = here.used
        here.used += len(make())

    def copies(self):
        return [
            pltpu.make_async_remote_copy(
                src_ref=src,
                dst_ref=dst,
                send_sem=self.here.send_sem.at[self.first + i],
                recv_sem=self.here.recv_sem.at[self.first + i],
                device_id=device,
                device_id_type=MESH,
            )
            for i, (src, dst, device) in enumerate(self.make())
        ]

    def start(self):
        for copy in self.copies():
            copy.start()

    def wait(self):
        for copy in self.copies():
            copy.wait()


def run(*works):
    works = list(works)
    while works:
        works = [work for work in works if next(work, "end") != "end"]


def gather_slots(here, part):
    along_z = here.step(
        lambda: [(part.at[here.slot], part.at[here.slot], here.at(z=z)) for z in here.z_peers()]
    )
    along_z.start()
    yield
    along_z.wait()

    def to_x():
        own = part.at[pl.ds(here.x * NZ, NZ)]
        return [(own, own, here.at(x=x)) for x in here.x_peers()]

    along_x = here.step(to_x)
    along_x.start()
    yield
    along_x.wait()


def gather_near(here, ref, skip=0):
    def near():
        own = ref.at[here.u, here.c]
        return [(own, own, here.at(u=u)) for u in here.u_peers()[skip:]] + [(own, own, here.at(c=1 - here.c))]

    step = here.step(near)
    step.start()
    yield
    step.wait()


def swap_rest(here, ref):
    def rest():
        copies = []
        for u in here.u_peers():
            block = ref.at[u, here.c]
            copies.append((block, block, here.at(c=1 - here.c)))
        return copies

    step = here.step(rest)
    step.start()
    yield
    step.wait()


def gather_targets(here, ref):
    yield from gather_near(here, ref)
    yield from swap_rest(here, ref)


def gram_sum(here, part, out, from_xy, from_z):
    def chunk(x, y):
        return pl.ds(pl.multiple_of((x * NY + y) * CHUNK, 8), CHUNK)

    spread = here.step(
        lambda: [
            (part.at[chunk(x, y)], from_xy.at[i], here.at(x=x, y=y)) for i, (x, y) in enumerate(here.xy_peers())
        ]
    )
    spread.start()
    yield
    spread.wait()
    total = part[chunk(here.x, here.y)]
    for i in range(NX * NY - 1):
        total = total + from_xy[i]
    from_z[here.z] = total
    along_z = here.step(lambda: [(from_z.at[here.z], from_z.at[here.z], here.at(z=z)) for z in here.z_peers()])
    along_z.start()
    yield
    along_z.wait()
    total = from_z[0]
    for i in range(1, NZ):
        total = total + from_z[i]
    out[here.u, here.c, chunk(here.x, here.y)] = total

    def to_u():
        own = out.at[here.u, here.c, chunk(here.x, here.y)]
        return [(own, own, here.at(u=u)) for u in here.u_peers()]

    along_u = here.step(to_u)
    along_u.start()
    yield
    along_u.wait()

    def to_xy():
        own = out.at[:, here.c, chunk(here.x, here.y)]
        return [(own, own, here.at(x=x, y=y)) for x, y in here.xy_peers()]

    across = here.step(to_xy)
    across.start()
    yield
    across.wait()
    swap = here.step(lambda: [(out.at[:, here.c], out.at[:, here.c], here.at(c=1 - here.c))])
    swap.start()
    yield
    swap.wait()


def gram_share(here, left, right):
    mask = lax.broadcasted_iota(jnp.int32, (COLS, PAIR), 1) // COLS == here.y
    whole = right[here.u].reshape(NC * COLS, PAIR)
    shares = []
    for d in range(3):
        rows = left[lax.rem(here.u + d, NU), here.c]
        shares.append(fine(jnp.where(mask, rows, 0.0), whole, NT))
    return jnp.concatenate(shares, axis=0)


def project(slots, feats, first, count):
    def group(i, total):
        index = lax.rem(first + i, NX)
        for z in range(NZ):
            at = pl.ds(pl.multiple_of((index * NZ + z) * PAIR, PAIR), PAIR)
            total = total + quick(slots[index * NZ + z], feats[:, at], NT)
        return total

    return lax.fori_loop(0, count, group, jnp.zeros((COLS, feats.shape[0]), f32))


def cosine(x):
    n = jnp.floor(x * 0.3183098861837907 + 0.5)
    r = ((x - n * 3.140625) - n * 0.0009670257568359375) - n * 6.2771141529083251953e-07
    half = n * 0.5
    sign = 1.0 - 4.0 * (half - jnp.floor(half))
    q = r * r
    poly = 1.0 / 479001600.0
    for term in (-1.0 / 3628800.0, 1.0 / 40320.0, -1.0 / 720.0, 1.0 / 24.0, -0.5, 1.0):
        poly = poly * q + term
    return sign * poly


def invert_blocks(blocks):
    count = BK // PN
    row = lax.broadcasted_iota(jnp.int32, (PN, BK), 0)
    lane = lax.broadcasted_iota(jnp.int32, (PN, BK), 1)
    mats = [[b[g * PN : (g + 1) * PN, :] for g in range(count)] for b in blocks]

    def wide(v, j):
        return jnp.broadcast_to(v[:, j : j + 1], (PN, BK))

    def tall(v, i):
        return jnp.broadcast_to(v[i : i + 1, :], (PN, BK))

    for p in range(count):
        base = p * PN
        inside = (lane >= base) & (lane < base + PN)
        reduced = []
        for m in mats:
            panel = m[p]
            cols = [wide(panel, base + k) for k in range(PN)]
            for i in range(PN):
                inv = 1.0 / tall(cols[i], i)
                here = row == i
                factor = jnp.where(here, 0.0, cols[i])
                src = jnp.where(lane == base + i, jnp.where(here, 1.0, 0.0), panel)
                pivot = tall(src, i) * inv
                panel = jnp.where(here, pivot, src - factor * pivot)
                for k in range(i + 1, PN):
                    top = tall(cols[k], i) * inv
                    cols[k] = jnp.where(here, top, cols[k] - factor * top)
            reduced.append(panel)
        for m, panel in zip(mats, reduced):
            rows = [tall(panel, k) for k in range(PN)]
            for g in [(p + 1 + g) % count for g in range(count - 1)]:
                acc = jnp.where(inside, 0.0, m[g])
                for k in range(PN):
                    acc = acc - wide(m[g], base + k) * rows[k]
                m[g] = acc
            m[p] = panel
    return [jnp.concatenate(m, axis=0) for m in mats]


def reduce_block(ref, k, at, hook):
    (inverse,) = invert_blocks([ref[at, at]])
    ref[at, at] = inverse
    hook()
    inverse = ref[at, at]
    rows = lax.broadcasted_iota(jnp.int32, (TOTAL, BK), 0)
    cols = lax.broadcasted_iota(jnp.int32, (BK, BK), 1)
    ref[at, at] = jnp.where(lax.broadcasted_iota(jnp.int32, (BK, BK), 0) == cols, 1.0, 0.0)
    head = fine(inverse, ref[at, :])
    left = jnp.where(rows // BK == k, 0.0, ref[:, at])
    ref[:, at] = jnp.zeros((TOTAL, BK), f32)
    ref[...] = ref[...] - fine(left, head)
    ref[at, :] = head


def invert(ref, hooks=None):
    steps = TOTAL // BK
    if hooks is None:

        def one(k, carry):
            reduce_block(ref, k, pl.ds(pl.multiple_of(k * BK, BK), BK), lambda: None)
            return carry

        lax.fori_loop(0, steps, one, 0)
    else:
        for k in range(steps):
            reduce_block(ref, k, pl.ds(k * BK, BK), hooks[2 * k])
            hooks[2 * k + 1]()


def assemble(gram, ref):
    for u in range(NU):
        for d in range(3):
            r = (u + d) % NU
            block = gram[u, :, d * COLS : (d + 1) * COLS, :].reshape(BK, BK)
            ref[r * BK : (r + 1) * BK, u * BK : (u + 1) * BK] = block
            if d == 1:
                ref[u * BK : (u + 1) * BK, r * BK : (r + 1) * BK] = block.T


def later(*works):
    def hook():
        for work in works:
            next(work, None)

    return hook


def kernel(
    total_samples, samples, omega, phase, right_side, out,
    feats, block, from_y, b_all, q_all, r_all, t_all, t_err, v_all, high, low, high_r, proj, proj_low, image, image_x, image_z, sum_x,
    sum_z, image_y, share_m, share_s, share_r, share_p, gram_sm, gram_r, gram_p, mxy, mz, sxy, sz, rxy, rz,
    pxy, pz, inv_sm, p_inv, m_high, m_low, m_full, r_full, alpha_t, beta_t, p_all, t1, send_sem, recv_sem,
):
    here = Place(send_sem, recv_sem)
    count, lanes = samples.shape[0], t_all.shape[-1]
    flat = (TOTAL, PAIR)
    here.greet()
    mine = lax.broadcasted_iota(jnp.int32, (COLS, PAIR), 1) // COLS == here.y
    turned = right_side[...].T
    block[...] = jnp.where(mine, jnp.concatenate([turned, turned], axis=1), 0.0)

    def features(first, chunks):
        width = 2 * PAIR

        def one(i, carry):
            at = pl.ds(pl.multiple_of((first + i) * width, width), width)
            feats[:, at] = cosine(quick(samples[...], omega[:, at]) + phase[:, at]).astype(bf16)
            return carry

        lax.fori_loop(0, chunks, one, 0)

    scope = jax.named_scope
    gram_s, gram_m = gram_sm.at[0], gram_sm.at[1]
    s_inv, m_inv = inv_sm.at[0], inv_sm.at[1]
    with scope("feat1"):
        features(0, 8)
    with scope("meet"):
        here.meet()
    pair = here.step(lambda: [(block, from_y, here.at(y=1 - here.y))])
    pair.start()
    with scope("feat2"):
        features(8, 4)
        t_all[...] = jnp.zeros_like(t_all)
        t_err[...] = jnp.zeros_like(t_err)
        v_all[...] = jnp.zeros_like(v_all)
    with scope("pairwait"):
        pair.wait()
        both = block[...] + from_y[...]
        b_all[here.u, here.c] = both
        high[here.slot] = both.astype(bf16)
        low[here.slot] = (both - both.astype(bf16).astype(f32)).astype(bf16)
    gather_high, gather_low = gather_slots(here, high), gather_slots(here, low)
    targets_b = gather_near(here, b_all)
    next(gather_high)
    next(targets_b)
    next(gather_low)
    with scope("feat3"):
        features(12, 4)
    with scope("waitb"):
        next(targets_b, None)
    rest_b = swap_rest(here, b_all)
    with scope("sharem"):
        share_m[...] = gram_share(here, b_all, b_all)
    sum_m = gram_sum(here, share_m, gram_m, mxy, mz)
    next(sum_m)
    next(rest_b)
    with scope("waithz"):
        next(gather_high)
    with scope("waitlz"):
        next(gather_low)
    with scope("proj1"):
        proj[...] = project(high, feats, here.x, 1)
        proj_low[...] = project(low, feats, here.x, 1)
    with scope("m_xy"):
        next(sum_m)
    with scope("waithx"):
        next(gather_high, None)
    with scope("proj2"):
        proj[...] = proj[...] + project(high, feats, here.x + 1, NX - 1)
        t_all[here.u, here.c, :, :count] = proj[...].astype(bf16)
    targets_t = gather_near(here, t_all)
    next(targets_t)

    with scope("image"):
        rounded = proj[...].astype(bf16)

        def image_group(i, carry):
            for z in range(NZ):
                at = pl.ds(pl.multiple_of((i * NZ + z) * PAIR, PAIR), PAIR)
                image[i * NZ + z] = quick(rounded, feats[:, at]).astype(bf16)
            return carry

        lax.fori_loop(0, NX, image_group, 0)

    def sum_of_image():
        def to_x():
            return [
                (image.at[pl.ds(x * NZ, NZ)], image_x.at[i], here.at(x=x)) for i, x in enumerate(here.x_peers())
            ]

        along_x = here.step(to_x)
        along_x.start()
        yield
        along_x.wait()
        total = image[pl.ds(here.x * NZ, NZ)].astype(f32)
        for i in range(NX - 1):
            total = total + image_x[i].astype(f32)
        sum_x[...] = total
        along_z = here.step(
            lambda: [(sum_x.at[z], image_z.at[i], here.at(z=z)) for i, z in enumerate(here.z_peers())]
        )
        along_z.start()
        yield
        along_z.wait()
        total = sum_x[here.z]
        for i in range(NZ - 1):
            total = total + image_z[i]
        sum_z[...] = total
        along_y = here.step(lambda: [(sum_z, image_y, here.at(y=1 - here.y))])
        along_y.start()
        yield
        along_y.wait()
        total = sum_z[...] + image_y[...]
        q_all[here.u, here.c] = total * (1.0 / total_samples) + RIDGE * b_all[here.u, here.c]
        yield from gather_targets(here, q_all)

    with scope("m_z"):
        next(sum_m)
    with scope("waitlx"):
        next(gather_low, None)
    with scope("proj3"):
        exact = proj[...] + (proj_low[...] + project(low, feats, here.x + 1, NX - 1))
        t_err[here.u, here.c, :, :count] = (exact - proj[...].astype(bf16).astype(f32)).astype(bf16)
    targets_e = gather_near(here, t_err, 1)
    next(targets_e)
    image_sum = sum_of_image()
    with scope("m_u"):
        next(sum_m)
    with scope("waitt"):
        next(targets_t, None)
    with scope("waite"):
        next(targets_e, None)
    with scope("shares"):
        right = t_all[here.u].reshape(NC * COLS, lanes)
        right_err = t_err[here.u].reshape(NC * COLS, lanes)
        for d in range(3):
            at = lax.rem(here.u + d, NU)
            value, err = t_all[at, here.c], t_err[at, here.c]
            cross = quick(err, right, NT) + quick(value, right_err, NT)
            rows = pl.ds(d * COLS, COLS)
            share_s[rows] = (quick(value, right, NT) + 0.5 * cross) * (1.0 / total_samples) + RIDGE * share_m[rows]
    sum_s = gram_sum(here, share_s, gram_s, sxy, sz)
    next(sum_s)
    next(image_sum)
    rest_t = swap_rest(here, t_all)
    next(rest_t)
    with scope("s_xy"):
        next(sum_s)
    with scope("m_xy2"):
        next(sum_m)
    with scope("s_z"):
        next(sum_s)
    with scope("image_x"):
        next(image_sum)
    with scope("s_u"):
        next(sum_s)
    with scope("m_end"):
        next(sum_m, None)
    with scope("s_xy2"):
        next(sum_s)
    with scope("s_end"):
        next(sum_s, None)

    mine_inv = inv_sm.at[here.c]
    with scope("assemble"):
        assemble(gram_sm.at[here.c], mine_inv)
    side, idle = later(image_sum), later()
    with scope("inverse1"):
        invert(mine_inv, [side, idle, side, idle, side, idle, side, idle])
    swap = here.step(lambda: [(inv_sm.at[here.c], inv_sm.at[here.c], here.at(c=1 - here.c))])
    swap.start()
    with scope("drain"):
        run(rest_b, rest_t, image_sum)
        assemble(gram_m, m_full)
    with scope("swap"):
        swap.wait()
    with scope("alpha"):
        alpha_t[...] = fine(m_full[...], s_inv[...])
    with scope("resid"):
        residual = b_all[...].reshape(flat) - fine(alpha_t[...], q_all[...].reshape(flat))
        r_all[...] = residual.reshape(r_all.shape)
        high_r[here.slot] = r_all[here.u, here.c].astype(bf16)
    gather_r = gather_slots(here, high_r)
    next(gather_r)
    with scope("sharer"):
        share_r[...] = gram_share(here, r_all, r_all)
    sum_r = gram_sum(here, share_r, gram_r, rxy, rz)
    next(sum_r)
    with scope("m_split"):
        m_high[...] = m_inv[...].astype(bf16)
        m_low[...] = (m_inv[...] - m_high[...].astype(f32)).astype(bf16)
    with scope("r_xy"):
        next(sum_r)
    with scope("r_gz"):
        next(gather_r)
    with scope("proj3"):
        proj[...] = project(high_r, feats, here.x, 1)
    with scope("r_z"):
        next(sum_r)
    with scope("r_gx"):
        next(gather_r, None)
    with scope("proj4"):
        v_own = proj[...] + project(high_r, feats, here.x + 1, NX - 1)
        v_all[here.u, here.c, :, :count] = v_own.astype(bf16)
    gather_v = gather_targets(here, v_all)
    next(gather_v)
    with scope("r_u"):
        next(sum_r)
    with scope("v_u"):
        next(gather_v)
    with scope("r_xy2"):
        next(sum_r)
    with scope("r_end"):
        run(sum_r, gather_v)

    with scope("beta"):
        assemble(gram_r, r_full)
        upper = r_full[...].astype(bf16)
        lower = (r_full[...] - upper.astype(f32)).astype(bf16)
        beta_t[...] = quick(upper, m_high[...]) + (quick(lower, m_high[...]) + quick(upper, m_low[...]))
    with scope("pdir"):
        p_all[...] = r_all[...].reshape(flat) + fine(beta_t[...], b_all[...].reshape(flat))
    with scope("tdir"):
        t_flat = t_all[...].reshape(TOTAL, lanes)
        upper = beta_t[...].astype(bf16)
        lower = (beta_t[...] - upper.astype(f32)).astype(bf16)
        moved = quick(upper, t_flat) + quick(lower, t_flat)
        t1[...] = (v_all[...].reshape(TOTAL, lanes).astype(f32) + moved).astype(bf16)
    with scope("sharep"):
        own = pl.ds(pl.multiple_of(here.u * 2 * COLS, 2 * COLS), 2 * COLS)
        right_p, right_t = p_all[own, :], t1[own, :]
        for d in range(3):
            at = pl.ds(pl.multiple_of((lax.rem(here.u + d, NU) * 2 + here.c) * COLS, COLS), COLS)
            gram = quick(t1[at, :], right_t, NT) * (1.0 / total_samples)
            share_p[pl.ds(d * COLS, COLS)] = gram + RIDGE * fine(jnp.where(mine, p_all[at, :], 0.0), right_p, NT)
    with scope("sump"):
        sum_p = gram_sum(here, share_p, gram_p, pxy, pz)
        next(sum_p)
        own = pl.ds(pl.multiple_of((here.u * 2 + here.c) * COLS, COLS), COLS)
        weights = fine(alpha_t[own, :], b_all[...].reshape(flat))
        run(sum_p)
    with scope("inverse2"):
        assemble(gram_p, p_inv)
        invert(p_inv)
    with scope("final"):
        last_t = fine(r_full[own, :], p_inv[...])
        weights = weights + fine(last_t, p_all[...])
        out[...] = jnp.where(here.y == 0, weights[:, :COLS], weights[:, COLS:]).T


def body(samples, omega, phase, right_side):
    count = samples.shape[0]
    total_samples = count * lax.axis_size("samp")
    vm = pltpu.VMEM
    all_feats = vm((NU, NC, COLS, PAIR), f32)
    all_samples = vm((NU, NC, COLS, 2 * PAIR), bf16)
    share = vm((GRAM, BK), f32)
    gram = vm((NU, NC, GRAM, BK), f32)
    sums = [vm((NX * NY - 1, CHUNK, BK), f32), vm((NZ, CHUNK, BK), f32)]
    slots = vm((SLOTS, COLS, PAIR), bf16)
    block = vm((COLS, PAIR), f32)
    full, half = vm((TOTAL, TOTAL), f32), vm((TOTAL, TOTAL), bf16)
    grams, fulls = vm((2, NU, NC, GRAM, BK), f32), vm((2, TOTAL, TOTAL), f32)
    scratch = [vm((count, omega.shape[1]), bf16), block, block, all_feats, all_feats, all_feats]
    scratch += [all_samples, all_samples, all_samples, slots, slots, slots, vm((COLS, count), f32), vm((COLS, count), f32)]
    scratch += [slots, vm((NX - 1, NZ, COLS, PAIR), bf16), vm((NZ - 1, COLS, PAIR), f32), vm((NZ, COLS, PAIR), f32)]
    scratch += [block, block, share, share, share, share, grams, gram, gram, *sums, *sums, *sums, *sums]
    scratch += [fulls, full, half, half, full, full, full, full, vm((TOTAL, PAIR), f32), vm((TOTAL, 2 * PAIR), bf16)]
    scratch += [pltpu.SemaphoreType.DMA((COPIES,))] * 2
    return pl.pallas_call(
        lambda *refs: kernel(total_samples, *refs),
        out_shape=jax.ShapeDtypeStruct(right_side.shape, f32),
        in_specs=[VMEM] * 4,
        out_specs=VMEM,
        scratch_shapes=scratch,
        name="cg",
        compiler_params=pltpu.CompilerParams(vmem_limit_bytes=60 * 2**20, collective_id=1, has_side_effects=True),
    )(samples, omega, phase.reshape(1, -1), right_side)


def solution(mesh):
    placed = (P("samp", None), P(), P(), P("samp", "tgt"))
    return jax.shard_map(body, mesh=mesh, in_specs=placed, out_specs=P("samp", "tgt"), check_vma=False)
```

```python
import jax
import jax.numpy as jnp
from jax import lax
from jax.experimental import pallas as pl
from jax.experimental.pallas import tpu as pltpu
from jax.sharding import PartitionSpec as P

f32 = jnp.float32
bf16 = jnp.bfloat16
MESH = pl.DeviceIdType.MESH
VMEM = pl.BlockSpec(memory_space=pltpu.VMEM)
RIDGE = 1.0

NX, NZ, NY, NU, NC = 4, 8, 2, 4, 2
COLS = 64
PAIR = 128
SLOTS = NX * NZ
CHUNK = 24
GRAM = CHUNK * NX * NY
TOTAL = NU * NC * COLS
BK = 128
PN = 8
COPIES = 340
NEAREST = (0, 1, 7, 2, 6, 3, 5, 4)
NT = (((1,), (1,)), ((), ()))
NN = (((1,), (0,)), ((), ()))


def fine(a, b, dims=NN):
    return lax.dot_general(a, b, dims, precision=lax.Precision.HIGHEST, preferred_element_type=f32)


def quick(a, b, dims=NN):
    return lax.dot_general(a, b, dims, preferred_element_type=f32)


class Place:
    def __init__(self, send_sem, recv_sem):
        samp, tgt = lax.axis_index("samp"), lax.axis_index("tgt")
        self.x, self.z, self.y = samp // 16, (samp % 16) // 2, samp % 2
        self.u, self.c = tgt // 2, tgt % 2
        self.slot = self.x * NZ + self.z
        self.send_sem, self.recv_sem, self.used = send_sem, recv_sem, 0

    def at(self, x=None, z=None, y=None, u=None, c=None):
        x, z, y = (own if new is None else new for own, new in ((self.x, x), (self.z, z), (self.y, y)))
        u, c = (own if new is None else new for own, new in ((self.u, u), (self.c, c)))
        return (x * 16 + z * 2 + y, u * 2 + c)

    def z_peers(self):
        return [lax.rem(self.z + d, NZ) for d in range(1, NZ)]

    def x_peers(self):
        return [lax.rem(self.x + d, NX) for d in range(1, NX)]

    def u_peers(self):
        return [lax.rem(self.u + d, NU) for d in range(1, NU)]

    def xy_peers(self):
        return [(lax.rem(self.x + d, NX), y) for d in range(NX) for y in (self.y, 1 - self.y)][1:]

    def greet(self):
        devices = [self.at(z=z) for z in self.z_peers()]
        devices += [self.at(x=x, y=y) for x, y in self.xy_peers()]
        devices += [self.at(u=u) for u in self.u_peers()] + [self.at(c=1 - self.c)]
        barrier = pltpu.get_barrier_semaphore()
        for device in devices:
            pl.semaphore_signal(barrier, inc=1, device_id=device, device_id_type=MESH)
        self.greeted = len(devices)

    def meet(self):
        pl.semaphore_wait(pltpu.get_barrier_semaphore(), self.greeted)

    def step(self, make):
        return Step(self, make)


class Step:
    def __init__(self, here, make):
        self.here, self.make = here, make
        self.first = here.used
        here.used += len(make())

    def copies(self, which):
        return [
            pltpu.make_async_remote_copy(
                src_ref=src,
                dst_ref=dst,
                send_sem=self.here.send_sem.at[self.first + i],
                recv_sem=self.here.recv_sem.at[self.first + i],
                device_id=device,
                device_id_type=MESH,
            )
            for i, (src, dst, device) in list(enumerate(self.make()))[which]
        ]

    def start(self, which=slice(None)):
        for copy in self.copies(which):
            copy.start()

    def wait(self, which=slice(None)):
        for copy in self.copies(which):
            copy.wait()


def run(*works):
    works = list(works)
    while works:
        works = [work for work in works if next(work, "end") != "end"]


def gather_slots(here, part):
    forward, back = 1, NX - 1

    def along(x, d):
        return lax.rem(x + d, NX)

    def slot(x, offset):
        return part.at[x * NZ + lax.rem(here.z + offset, NZ)]

    def to_z():
        own = slot(here.x, 0)
        return [(own, own, here.at(z=lax.rem(here.z + NZ - offset, NZ))) for offset in NEAREST[1:]]

    def to_x():
        blocks = [slot(here.x, offset) for offset in NEAREST]
        return [(block, block, here.at(x=along(here.x, d))) for block in blocks for d in (forward, back)]

    def to_last():
        copies = []
        for i, offset in enumerate(NEAREST):
            d = (forward, back)[i % 2]
            block = slot(along(here.x, NX - d), offset)
            copies.append((block, block, here.at(x=along(here.x, d))))
        return copies

    z_step, x_step, last_step = here.step(to_z), here.step(to_x), here.step(to_last)
    z_step.start()
    x_step.start(slice(0, 2))
    yield
    for i in range(1, NZ):
        z_step.wait(slice(i - 1, i))
        x_step.start(slice(2 * i, 2 * i + 2))
    yield
    for i in range(NZ):
        x_step.wait(slice(2 * i, 2 * i + 2))
        last_step.start(slice(i, i + 1))
    yield
    last_step.wait()


def gather_near(here, ref, skip=0):
    def near():
        own = ref.at[here.u, here.c]
        return [(own, own, here.at(u=u)) for u in here.u_peers()[skip:]] + [(own, own, here.at(c=1 - here.c))]

    step = here.step(near)
    step.start()
    yield
    step.wait()


def swap_rest(here, ref):
    def rest():
        copies = []
        for u in here.u_peers():
            block = ref.at[u, here.c]
            copies.append((block, block, here.at(c=1 - here.c)))
        return copies

    step = here.step(rest)
    step.start()
    yield
    step.wait()


def gather_targets(here, ref):
    yield from gather_near(here, ref)
    yield from swap_rest(here, ref)


def gram_sum(here, part, out, from_xy, from_z):
    def chunk(x, y):
        return pl.ds(pl.multiple_of((x * NY + y) * CHUNK, 8), CHUNK)

    spread = here.step(
        lambda: [
            (part.at[chunk(x, y)], from_xy.at[i], here.at(x=x, y=y)) for i, (x, y) in enumerate(here.xy_peers())
        ]
    )
    spread.start()
    yield
    spread.wait()
    total = part[chunk(here.x, here.y)]
    for i in range(NX * NY - 1):
        total = total + from_xy[i]
    from_z[here.z] = total
    along_z = here.step(lambda: [(from_z.at[here.z], from_z.at[here.z], here.at(z=z)) for z in here.z_peers()])
    along_z.start()
    yield
    along_z.wait()
    total = from_z[0]
    for i in range(1, NZ):
        total = total + from_z[i]
    out[here.u, here.c, chunk(here.x, here.y)] = total

    def block(d):
        return out.at[lax.rem(here.u + d, NU), here.c, chunk(here.x, here.y)]

    near = (1, 3, 2)
    u_step = here.step(lambda: [(block(0), block(0), here.at(u=lax.rem(here.u + NU - d, NU))) for d in near])
    xy_step = here.step(
        lambda: [(block(d), block(d), here.at(x=x, y=y)) for d in (0, *near) for x, y in here.xy_peers()]
    )
    peers = NX * NY - 1
    u_step.start()
    xy_step.start(slice(0, peers))
    yield
    for i in range(1, NU):
        u_step.wait(slice(i - 1, i))
        xy_step.start(slice(i * peers, (i + 1) * peers))
    yield
    xy_step.wait()
    swap = here.step(lambda: [(out.at[:, here.c], out.at[:, here.c], here.at(c=1 - here.c))])
    swap.start()
    yield
    swap.wait()


def gram_share(here, left, right):
    mask = lax.broadcasted_iota(jnp.int32, (COLS, PAIR), 1) // COLS == here.y
    whole = right[here.u].reshape(NC * COLS, PAIR)
    shares = []
    for d in range(3):
        rows = left[lax.rem(here.u + d, NU), here.c]
        shares.append(fine(jnp.where(mask, rows, 0.0), whole, NT))
    return jnp.concatenate(shares, axis=0)


def project(slots, feats, first, count):
    def group(i, total):
        index = lax.rem(first + i, NX)
        for z in range(NZ):
            at = pl.ds(pl.multiple_of((index * NZ + z) * PAIR, PAIR), PAIR)
            total = total + quick(slots[index * NZ + z], feats[:, at], NT)
        return total

    return lax.fori_loop(0, count, group, jnp.zeros((COLS, feats.shape[0]), f32))


def cosine(x):
    n = jnp.floor(x * 0.3183098861837907 + 0.5)
    r = ((x - n * 3.140625) - n * 0.0009670257568359375) - n * 6.2771141529083251953e-07
    half = n * 0.5
    sign = 1.0 - 4.0 * (half - jnp.floor(half))
    q = r * r
    poly = 1.0 / 479001600.0
    for term in (-1.0 / 3628800.0, 1.0 / 40320.0, -1.0 / 720.0, 1.0 / 24.0, -0.5, 1.0):
        poly = poly * q + term
    return sign * poly


def invert_blocks(blocks):
    count = BK // PN
    row = lax.broadcasted_iota(jnp.int32, (PN, BK), 0)
    lane = lax.broadcasted_iota(jnp.int32, (PN, BK), 1)
    mats = [[b[g * PN : (g + 1) * PN, :] for g in range(count)] for b in blocks]

    def wide(v, j):
        return jnp.broadcast_to(v[:, j : j + 1], (PN, BK))

    def tall(v, i):
        return jnp.broadcast_to(v[i : i + 1, :], (PN, BK))

    for p in range(count):
        base = p * PN
        inside = (lane >= base) & (lane < base + PN)
        reduced = []
        for m in mats:
            panel = m[p]
            cols = [wide(panel, base + k) for k in range(PN)]
            for i in range(PN):
                inv = 1.0 / tall(cols[i], i)
                here = row == i
                factor = jnp.where(here, 0.0, cols[i])
                src = jnp.where(lane == base + i, jnp.where(here, 1.0, 0.0), panel)
                pivot = tall(src, i) * inv
                panel = jnp.where(here, pivot, src - factor * pivot)
                for k in range(i + 1, PN):
                    top = tall(cols[k], i) * inv
                    cols[k] = jnp.where(here, top, cols[k] - factor * top)
            reduced.append(panel)
        for m, panel in zip(mats, reduced):
            rows = [tall(panel, k) for k in range(PN)]
            for g in [(p + 1 + g) % count for g in range(count - 1)]:
                acc = jnp.where(inside, 0.0, m[g])
                for k in range(PN):
                    acc = acc - wide(m[g], base + k) * rows[k]
                m[g] = acc
            m[p] = panel
    return [jnp.concatenate(m, axis=0) for m in mats]


def reduce_block(ref, k, at, hook):
    (inverse,) = invert_blocks([ref[at, at]])
    ref[at, at] = inverse
    hook()
    inverse = ref[at, at]
    rows = lax.broadcasted_iota(jnp.int32, (TOTAL, BK), 0)
    cols = lax.broadcasted_iota(jnp.int32, (BK, BK), 1)
    ref[at, at] = jnp.where(lax.broadcasted_iota(jnp.int32, (BK, BK), 0) == cols, 1.0, 0.0)
    head = fine(inverse, ref[at, :])
    left = jnp.where(rows // BK == k, 0.0, ref[:, at])
    ref[:, at] = jnp.zeros((TOTAL, BK), f32)
    ref[...] = ref[...] - fine(left, head)
    ref[at, :] = head


def invert(ref, hooks=()):
    peeled = len(hooks) // 2
    for k in range(peeled):
        reduce_block(ref, k, pl.ds(k * BK, BK), hooks[2 * k])
        hooks[2 * k + 1]()

    def one(k, carry):
        reduce_block(ref, k, pl.ds(pl.multiple_of(k * BK, BK), BK), lambda: None)
        return carry

    lax.fori_loop(peeled, TOTAL // BK, one, 0)


def assemble(gram, ref):
    for u in range(NU):
        for d in range(3):
            r = (u + d) % NU
            block = gram[u, :, d * COLS : (d + 1) * COLS, :].reshape(BK, BK)
            ref[r * BK : (r + 1) * BK, u * BK : (u + 1) * BK] = block
            if d == 1:
                ref[u * BK : (u + 1) * BK, r * BK : (r + 1) * BK] = block.T


def later(*works):
    def hook():
        for work in works:
            next(work, None)

    return hook


def kernel(
    total_samples, samples, omega, phase, right_side, out,
    feats, block, from_y, b_all, q_all, r_all, t_all, t_err, v_all, high, low, high_r, proj, proj_low, image, image_x, image_z, sum_x,
    sum_z, image_y, share_m, share_s, share_r, share_p, gram_sm, gram_r, gram_p, mxy, mz, sxy, sz, rxy, rz,
    pxy, pz, inv_sm, p_inv, m_high, m_low, m_full, r_full, alpha_t, beta_t, p_all, t1, send_sem, recv_sem,
):
    here = Place(send_sem, recv_sem)
    count, lanes = samples.shape[0], t_all.shape[-1]
    flat = (TOTAL, PAIR)
    here.greet()
    mine = lax.broadcasted_iota(jnp.int32, (COLS, PAIR), 1) // COLS == here.y
    turned = right_side[...].T
    block[...] = jnp.where(mine, jnp.concatenate([turned, turned], axis=1), 0.0)

    def features(first, chunks):
        width = 2 * PAIR

        def one(i, carry):
            at = pl.ds(pl.multiple_of((first + i) * width, width), width)
            feats[:, at] = cosine(quick(samples[...], omega[:, at]) + phase[:, at]).astype(bf16)
            return carry

        lax.fori_loop(0, chunks, one, 0)

    scope = jax.named_scope
    gram_s, gram_m = gram_sm.at[0], gram_sm.at[1]
    s_inv, m_inv = inv_sm.at[0], inv_sm.at[1]
    with scope("feat1"):
        features(0, 8)
    with scope("meet"):
        here.meet()
    pair = here.step(lambda: [(block, from_y, here.at(y=1 - here.y))])
    pair.start()
    with scope("feat2"):
        features(8, 4)
        t_all[...] = jnp.zeros_like(t_all)
        t_err[...] = jnp.zeros_like(t_err)
        v_all[...] = jnp.zeros_like(v_all)
    with scope("pairwait"):
        pair.wait()
        both = block[...] + from_y[...]
        b_all[here.u, here.c] = both
        high[here.slot] = both.astype(bf16)
        low[here.slot] = (both - both.astype(bf16).astype(f32)).astype(bf16)
    gather_high, gather_low = gather_slots(here, high), gather_slots(here, low)
    targets_b = gather_near(here, b_all)
    next(gather_high)
    next(targets_b)
    next(gather_low)
    with scope("feat3"):
        features(12, 4)
    with scope("waitb"):
        next(targets_b, None)
    rest_b = swap_rest(here, b_all)
    with scope("sharem"):
        share_m[...] = gram_share(here, b_all, b_all)
    sum_m = gram_sum(here, share_m, gram_m, mxy, mz)
    next(sum_m)
    next(rest_b)
    with scope("waithz"):
        next(gather_high)
    with scope("waitlz"):
        next(gather_low)
    with scope("proj1"):
        proj[...] = project(high, feats, here.x, 1)
        proj_low[...] = project(low, feats, here.x, 1)
    with scope("waithx"):
        next(gather_high)
    with scope("proj2"):
        sides = project(high, feats, here.x + 1, 1) + project(high, feats, here.x + 3, 1)
        proj[...] = proj[...] + sides
    with scope("m_xy"):
        next(sum_m)
    with scope("waitlx"):
        next(gather_low)
    with scope("waithx2"):
        next(gather_high, None)
    with scope("proj2b"):
        proj[...] = proj[...] + project(high, feats, here.x + 2, 1)
        t_all[here.u, here.c, :, :count] = proj[...].astype(bf16)
    targets_t = gather_near(here, t_all)
    next(targets_t)
    with scope("proj3"):
        sides = project(low, feats, here.x + 1, 1) + project(low, feats, here.x + 3, 1)
        proj_low[...] = proj_low[...] + sides
    with scope("waitlx2"):
        next(gather_low, None)
    with scope("proj3b"):
        exact = proj[...] + (proj_low[...] + project(low, feats, here.x + 2, 1))
        t_err[here.u, here.c, :, :count] = (exact - proj[...].astype(bf16).astype(f32)).astype(bf16)
    targets_e = gather_near(here, t_err, 1)
    next(targets_e)
    with scope("m_z"):
        next(sum_m)

    with scope("image"):
        rounded = proj[...].astype(bf16)

        def image_group(i, carry):
            for z in range(NZ):
                at = pl.ds(pl.multiple_of((i * NZ + z) * PAIR, PAIR), PAIR)
                image[i * NZ + z] = quick(rounded, feats[:, at]).astype(bf16)
            return carry

        lax.fori_loop(0, NX, image_group, 0)

    def sum_of_image():
        def to_x():
            return [
                (image.at[pl.ds(x * NZ, NZ)], image_x.at[i], here.at(x=x)) for i, x in enumerate(here.x_peers())
            ]

        along_x = here.step(to_x)
        along_x.start()
        yield
        along_x.wait()
        total = image[pl.ds(here.x * NZ, NZ)].astype(f32)
        for i in range(NX - 1):
            total = total + image_x[i].astype(f32)
        sum_x[...] = total
        along_z = here.step(
            lambda: [(sum_x.at[z], image_z.at[i], here.at(z=z)) for i, z in enumerate(here.z_peers())]
        )
        along_z.start()
        yield
        along_z.wait()
        total = sum_x[here.z]
        for i in range(NZ - 1):
            total = total + image_z[i]
        sum_z[...] = total
        along_y = here.step(lambda: [(sum_z, image_y, here.at(y=1 - here.y))])
        along_y.start()
        yield
        along_y.wait()
        total = sum_z[...] + image_y[...]
        q_all[here.u, here.c] = total * (1.0 / total_samples) + RIDGE * b_all[here.u, here.c]
        yield from gather_targets(here, q_all)

    image_sum = sum_of_image()
    with scope("waitt"):
        next(targets_t, None)
    with scope("waite"):
        next(targets_e, None)
    with scope("shares"):
        right = t_all[here.u].reshape(NC * COLS, lanes)
        right_err = t_err[here.u].reshape(NC * COLS, lanes)
        for d in range(3):
            at = lax.rem(here.u + d, NU)
            value, err = t_all[at, here.c], t_err[at, here.c]
            cross = quick(err, right, NT) + quick(value, right_err, NT)
            rows = pl.ds(d * COLS, COLS)
            share_s[rows] = (quick(value, right, NT) + 0.5 * cross) * (1.0 / total_samples) + RIDGE * share_m[rows]
    sum_s = gram_sum(here, share_s, gram_s, sxy, sz)
    next(sum_s)
    with scope("m_u"):
        next(sum_m)
    next(image_sum)
    rest_t = swap_rest(here, t_all)
    next(rest_t)
    with scope("s_xy"):
        next(sum_s)
    with scope("s_z"):
        next(sum_s)
    with scope("m_xy2"):
        next(sum_m)
    with scope("s_u"):
        next(sum_s)
    with scope("image_x"):
        next(image_sum)
    with scope("m_end"):
        next(sum_m, None)
    with scope("s_xy2"):
        next(sum_s)
    with scope("s_end"):
        next(sum_s, None)

    mine_inv = inv_sm.at[here.c]
    with scope("assemble"):
        assemble(gram_sm.at[here.c], mine_inv)
    side, idle = later(image_sum), later()
    with scope("inverse1"):
        invert(mine_inv, [side, idle, side, idle])
    swap = here.step(lambda: [(inv_sm.at[here.c], inv_sm.at[here.c], here.at(c=1 - here.c))])
    swap.start()
    with scope("drain"):
        next(image_sum)
        run(rest_b, rest_t)
        assemble(gram_m, m_full)
    with scope("swap"):
        swap.wait()
    with scope("alpha"):
        alpha_t[...] = fine(m_full[...], s_inv[...])
    with scope("resid"):
        run(image_sum)
        residual = b_all[...].reshape(flat) - fine(alpha_t[...], q_all[...].reshape(flat))
        r_all[...] = residual.reshape(r_all.shape)
        high_r[here.slot] = r_all[here.u, here.c].astype(bf16)
    gather_r = gather_slots(here, high_r)
    next(gather_r)
    with scope("sharer"):
        share_r[...] = gram_share(here, r_all, r_all)
    sum_r = gram_sum(here, share_r, gram_r, rxy, rz)
    next(sum_r)
    with scope("m_split"):
        m_high[...] = m_inv[...].astype(bf16)
        m_low[...] = (m_inv[...] - m_high[...].astype(f32)).astype(bf16)
    with scope("r_xy"):
        next(sum_r)
    with scope("r_gz"):
        next(gather_r)
    with scope("proj4"):
        proj[...] = project(high_r, feats, here.x, 1)
    with scope("r_z"):
        next(sum_r)
    with scope("r_gx"):
        next(gather_r)
    with scope("proj5"):
        sides = project(high_r, feats, here.x + 1, 1) + project(high_r, feats, here.x + 3, 1)
        proj[...] = proj[...] + sides
    with scope("r_gx2"):
        next(gather_r, None)
    with scope("proj6"):
        v_all[here.u, here.c, :, :count] = (proj[...] + project(high_r, feats, here.x + 2, 1)).astype(bf16)
    gather_v = gather_targets(here, v_all)
    next(gather_v)
    with scope("r_u"):
        next(sum_r)
    with scope("v_u"):
        next(gather_v)
    with scope("r_xy2"):
        next(sum_r)
    with scope("r_end"):
        run(sum_r, gather_v)

    with scope("beta"):
        assemble(gram_r, r_full)
        upper = r_full[...].astype(bf16)
        lower = (r_full[...] - upper.astype(f32)).astype(bf16)
        beta_t[...] = quick(upper, m_high[...]) + (quick(lower, m_high[...]) + quick(upper, m_low[...]))
    with scope("pdir"):
        p_all[...] = r_all[...].reshape(flat) + fine(beta_t[...], b_all[...].reshape(flat))
    with scope("tdir"):
        t_flat = t_all[...].reshape(TOTAL, lanes)
        upper = beta_t[...].astype(bf16)
        lower = (beta_t[...] - upper.astype(f32)).astype(bf16)
        moved = quick(upper, t_flat) + quick(lower, t_flat)
        t1[...] = (v_all[...].reshape(TOTAL, lanes).astype(f32) + moved).astype(bf16)
    with scope("sharep"):
        own = pl.ds(pl.multiple_of(here.u * 2 * COLS, 2 * COLS), 2 * COLS)
        right_p, right_t = p_all[own, :], t1[own, :]
        for d in range(3):
            at = pl.ds(pl.multiple_of((lax.rem(here.u + d, NU) * 2 + here.c) * COLS, COLS), COLS)
            gram = quick(t1[at, :], right_t, NT) * (1.0 / total_samples)
            share_p[pl.ds(d * COLS, COLS)] = gram + RIDGE * fine(jnp.where(mine, p_all[at, :], 0.0), right_p, NT)
    with scope("sump"):
        sum_p = gram_sum(here, share_p, gram_p, pxy, pz)
        next(sum_p)
        own = pl.ds(pl.multiple_of((here.u * 2 + here.c) * COLS, COLS), COLS)
        weights = fine(alpha_t[own, :], b_all[...].reshape(flat))
        run(sum_p)
    with scope("inverse2"):
        assemble(gram_p, p_inv)
        invert(p_inv)
    with scope("final"):
        last_t = fine(r_full[own, :], p_inv[...])
        weights = weights + fine(last_t, p_all[...])
        out[...] = jnp.where(here.y == 0, weights[:, :COLS], weights[:, COLS:]).T


def body(samples, omega, phase, right_side):
    count = samples.shape[0]
    total_samples = count * lax.axis_size("samp")
    vm = pltpu.VMEM
    all_feats = vm((NU, NC, COLS, PAIR), f32)
    all_samples = vm((NU, NC, COLS, 2 * PAIR), bf16)
    share = vm((GRAM, BK), f32)
    gram = vm((NU, NC, GRAM, BK), f32)
    sums = [vm((NX * NY - 1, CHUNK, BK), f32), vm((NZ, CHUNK, BK), f32)]
    slots = vm((SLOTS, COLS, PAIR), bf16)
    block = vm((COLS, PAIR), f32)
    full, half = vm((TOTAL, TOTAL), f32), vm((TOTAL, TOTAL), bf16)
    grams, fulls = vm((2, NU, NC, GRAM, BK), f32), vm((2, TOTAL, TOTAL), f32)
    scratch = [vm((count, omega.shape[1]), bf16), block, block, all_feats, all_feats, all_feats]
    scratch += [all_samples, all_samples, all_samples, slots, slots, slots, vm((COLS, count), f32), vm((COLS, count), f32)]
    scratch += [slots, vm((NX - 1, NZ, COLS, PAIR), bf16), vm((NZ - 1, COLS, PAIR), f32), vm((NZ, COLS, PAIR), f32)]
    scratch += [block, block, share, share, share, share, grams, gram, gram, *sums, *sums, *sums, *sums]
    scratch += [fulls, full, half, half, full, full, full, full, vm((TOTAL, PAIR), f32), vm((TOTAL, 2 * PAIR), bf16)]
    scratch += [pltpu.SemaphoreType.DMA((COPIES,))] * 2
    return pl.pallas_call(
        lambda *refs: kernel(total_samples, *refs),
        out_shape=jax.ShapeDtypeStruct(right_side.shape, f32),
        in_specs=[VMEM] * 4,
        out_specs=VMEM,
        scratch_shapes=scratch,
        name="cg",
        compiler_params=pltpu.CompilerParams(vmem_limit_bytes=60 * 2**20, collective_id=1, has_side_effects=True),
    )(samples, omega, phase.reshape(1, -1), right_side)


def solution(mesh):
    placed = (P("samp", None), P(), P(), P("samp", "tgt"))
    return jax.shard_map(body, mesh=mesh, in_specs=placed, out_specs=P("samp", "tgt"), check_vma=False)
```
